32 devices in a mesh: groups: 2 (over y), ep: 4 (over z), tp: 2 (over x), dp: 2 (over core).
Axes of the slice: x: 2, y: 2, z: 4, core: 2. Of those that a mesh axis runs over, the one named last changes fastest.
Arguments:
- tokens: bfloat16 [512, 1536], P(('groups', 'ep', 'tp', 'dp')), parts along dimension 0, may hold values from -6 to 6
- expert_ids: int32 [512, 4], P(('groups', 'ep', 'tp', 'dp')), parts along dimension 0, may hold values from 0 to 7, all different within a row; in each aligned block of 16 rows (0 to 15, 16 to 31, ...) at most 16 rows name the same one
- gate_weights: float32 [512, 4], P(('groups', 'ep', 'tp', 'dp')), parts along dimension 0, may hold values from 0.1 to 1
- w_gate: bfloat16 [8, 1536, 1536], P(('ep', 'dp'), None, 'tp'), may hold values from -0.15625 to 0.15625
- w_up: bfloat16 [8, 1536, 1536], P(('ep', 'dp'), None, 'tp'), may hold values from -0.15625 to 0.15625
- w_down: bfloat16 [8, 1536, 1536], P(('ep', 'dp'), None, 'tp'), may hold values from -0.15625 to 0.15625
Outputs:
- mixed: bfloat16 [512, 1536], P(('groups', 'ep', 'tp', 'dp')), parts along dimension 0
- expert_loads: int32 [16], P('groups'), parts along dimension 0
The draws below stay inside these ranges and needn't reach their ends.
There are 2 independent parts, one for each index of `groups`. The reference program is written for one: setup_inputs(seed, part) draws one part's arguments, and reference() takes and returns one part's arrays. A program takes and returns all parts, laid end to end along the dimension named above; an argument that names none is the same for every part. Nothing has to cross between parts.
Inputs may be any that keep to these rules, and one draw needn't show every extreme that they name: `expert_ids`: each row names 4 different experts. In each aligned block of 16 rows (the rows of one device) no expert is named by more than 16 rows, and in some blocks one expert is named by exactly 16 rows.
All inputs are finite; a program needn't handle non-finite values.
Results may differ from the reference program's by a relative error of at most 0.0057.
Values may be sent and summed in bfloat16 or wider, within the bound.
A program may use at most 64 MiB of HBM per device.

```python
import math
import jax
import jax.numpy as jnp
import numpy as np
from jax import lax

D = 1536
FF = 1536
TOP = 4
TOK_DEV = 16
EXPERTS = 8
CAP = 16
TOKENS = 256


def level_of(rng, shape, shards, low, largest):
    gain = 1.0
    for position, parts in shards:
        steps = jax.random.uniform(jax.random.fold_in(jax.random.fold_in(rng, 6), position), (parts,), jnp.float32, low / len(shards), largest / len(shards))
        gain = gain * jnp.repeat(jnp.exp(steps), shape[position] // parts).reshape((-1,) + (1,) * (len(shape) - 1 - position))
    return gain


def shared_out(own_key, own, number, rows, amount, top, bound, slope):
    sequence = jax.random.permutation(own_key, amount)
    crowded, ordinary = portions_of(amount, rows * top, bound, slope, True), portions_of(amount, rows * top, bound, slope, False)
    places = jnp.arange(amount)

    def named(lengths, offset_by):
        used = int((lengths > 0).sum())
        fixed = max(1, used // 4)
        passed = fixed + (places - fixed + offset_by * (used - fixed)) % max(1, amount - fixed)
        return jnp.zeros((amount,), jnp.int32).at[sequence[jnp.where(places < fixed, places, passed)]].set(jnp.asarray(lengths, jnp.int32))

    lengths = jnp.where(number % 4 == 0, named(crowded, number // 4), named(ordinary, number - number // 4 - 1))
    mixed = jax.random.permutation(jax.random.fold_in(own, 3), amount)
    donor, receiver = mixed[0:amount // 2 * 2:2], mixed[1:amount // 2 * 2:2]
    slack = jnp.minimum(lengths[donor] - 1, bound - lengths[receiver]) // 2
    slack = jnp.where((donor == sequence[0]) | (receiver == sequence[0]) | (lengths[receiver] == 0), 0, jnp.maximum(slack, 0))
    passed = jax.random.randint(jax.random.fold_in(own, 4), (amount // 2,), 0, 1 << 20) % (slack + 1)
    lengths = lengths.at[donor].add(-passed).at[receiver].add(passed)
    labels = jnp.searchsorted(jnp.cumsum(lengths), jnp.arange(rows * top), side="right").astype(jnp.int32)
    table = labels.reshape(top, rows).T
    table = table[jax.random.permutation(jax.random.fold_in(own, 1), rows)]
    offset_by = jax.random.randint(jax.random.fold_in(own, 2), (rows, 1), 0, top)
    return jnp.take_along_axis(table, (jnp.arange(top)[None, :] + offset_by) % top, axis=1)


def portions_of(amount, total, limit, skew, full):
    portions = [(1 << 20) // math.isqrt(rank ** skew) + 1 for rank in range(1, amount + 1)]
    largest = limit if full else min(limit, max(-(-total // amount), total * portions[0] // sum(portions)))
    least = 1 if total - largest >= amount - 1 else 0
    given, surplus = [largest] + [least] * (amount - 1), total - largest - least * (amount - 1)
    while surplus > 0:
        candidates = [i for i in range(1, amount) if given[i] < largest] or [i for i in range(1, amount) if given[i] < limit]
        pool, left = sum([portions[i] for i in candidates]), surplus
        for i in candidates:
            more = min(limit - given[i], max(1, left * portions[i] // pool), surplus)
            given[i] = given[i] + more
            surplus = surplus - more
    return np.array(given)


def bell_draw(own_key, shape, spread, reach, cuts=(), held_as=jnp.bfloat16):
    values = jax.random.normal(own_key, shape, jnp.float32) * spread
    if len(cuts) > 0:
        values = level_of(own_key, shape, cuts, -0.22, 0.18) * values
    return jnp.clip(values, min=-reach, max=reach).astype(held_as)


def setup_inputs(seed: int = 0, part: int = 0) -> dict:
    key_of = jax.random.split(jax.random.key(seed), 7)
    own_keys = jax.random.split(jax.random.fold_in(key_of[6], part), 7)
    tokens = bell_draw(own_keys[0], (TOKENS, D), 1.0, 6.0, ((0, 16),))
    expert_ids_keys = jax.random.split(jax.random.fold_in(own_keys[1], 1), TOKENS // TOK_DEV)
    expert_ids_turns = jax.random.permutation(jax.random.fold_in(own_keys[1], 3), TOKENS // TOK_DEV)
    expert_ids = jax.vmap(lambda own, number: shared_out(jax.random.fold_in(own_keys[1], 2), own, number, TOK_DEV, EXPERTS, TOP, CAP, 2))(expert_ids_keys, expert_ids_turns).reshape((TOKENS, TOP))
    gate_weights = jnp.clip(0.1 + 0.9 * jax.random.uniform(own_keys[2], (TOKENS, TOP), jnp.float32) ** level_of(own_keys[2], (TOKENS, TOP), ((0, 16),), -0.2, 0.2), 0.1, 1.0)
    w_gate = bell_draw(key_of[3], (EXPERTS, D, FF), D ** -0.5, 0.15625, ((0, 8), (2, 2)))
    w_up = bell_draw(key_of[4], (EXPERTS, D, FF), D ** -0.5, 0.15625, ((0, 8), (2, 2)))
    w_down = bell_draw(key_of[5], (EXPERTS, D, FF), FF ** -0.5, 0.15625, ((0, 8), (2, 2)))
    return {"tokens": tokens, "expert_ids": expert_ids, "gate_weights": gate_weights, "w_gate": w_gate, "w_up": w_up, "w_down": w_down}


def reference(tokens, expert_ids, gate_weights, w_gate, w_up, w_down):
    pair_ids = expert_ids.reshape(-1).astype(jnp.int32)
    pair_count = pair_ids.shape[0]
    expert_range = jnp.arange(EXPERTS, dtype=jnp.int32)
    onehot = (pair_ids[:, None] == expert_range[None, :]).astype(jnp.int32)
    expert_loads = jnp.sum(onehot, axis=0).astype(jnp.int32)
    earlier = (jnp.cumsum(onehot, axis=0).astype(jnp.int32) - onehot) * onehot
    slot_ranks = jnp.sum(earlier, axis=1).astype(jnp.int32)
    holder = (TOKENS // TOK_DEV) * CAP
    token_of_pair = (jnp.arange(pair_count, dtype=jnp.int32) // TOP).astype(jnp.int32)
    table = jnp.full((EXPERTS, holder), TOKENS, jnp.int32).at[pair_ids, slot_ranks].set(token_of_pair)
    padded = jnp.concatenate([tokens, jnp.zeros((1, D), jnp.bfloat16)], axis=0)

    def one_expert(packed):
        row_index, gate_part, up_part, down_part = packed
        token_rows = padded[row_index]
        gate_value = jnp.dot(token_rows, gate_part, preferred_element_type=jnp.float32)
        up_value = jnp.dot(token_rows, up_part, preferred_element_type=jnp.float32)
        hidden = (jax.nn.silu(gate_value) * up_value).astype(jnp.bfloat16)
        result = lax.dot_general(hidden, down_part, (((1,), (1,)), ((), ())), preferred_element_type=jnp.float32)
        return result.astype(jnp.bfloat16)

    outputs = lax.map(one_expert, (table, w_gate, w_up, w_down))
    picked = outputs[pair_ids, slot_ranks].reshape(TOKENS, TOP, D)
    mixed = jnp.sum(gate_weights[:, :, None] * picked.astype(jnp.float32), axis=1)
    return mixed.astype(jnp.bfloat16), expert_loads
```

```python
import functools

import jax
import jax.numpy as jnp
from jax import lax
from jax.experimental import pallas as pl
from jax.experimental.pallas import tpu as pltpu
from jax.sharding import PartitionSpec as P

MESH = pl.DeviceIdType.MESH
LANES = 128
STRIP = 512


def nearest_order(ep_count):
    rows = []
    for own in range(ep_count):
        others = [z for z in range(ep_count) if z != own]
        rows.append(sorted(others, key=lambda z: (abs(z - own), z)))
    return rows


def pick(rows, own, position):
    value = jnp.int32(rows[0][position])
    for index in range(1, len(rows)):
        value = jnp.where(own == index, jnp.int32(rows[index][position]), value)
    return value


def layer_kernel(
    sizes,
    tok_hbm, ids_hbm, gw_hbm, wg_hbm, wu_hbm, wd_hbm,
    out_ref, loads_ref,
    xall, ids_v, gw_v, wg, wu, wd, resf, resb, drecv, xsend, xrecv, zsend, zrecv,
    local_sem, az_s, az_r, ax_s, ax_r, ad_s, ad_r, rd_s, rd_r, rx_s, rx_r, rz_s, rz_r,
):
    ep, tp, dp, rows, width, top, experts = sizes
    z, x, c = lax.axis_index("ep"), lax.axis_index("tp"), lax.axis_index("dp")
    order = nearest_order(ep)
    z_peers = [pick(order, z, k) for k in range(ep - 1)]
    x_peers = [lax.rem(x + k, tp) for k in range(1, tp)]
    c_peers = [lax.rem(c + k, dp) for k in range(1, dp)]

    tok_in = pltpu.make_async_copy(
        tok_hbm, xall.at[x, c, z, :, pl.ds(0, width)], local_sem.at[0]
    )
    ids_in = pltpu.make_async_copy(ids_hbm, ids_v, local_sem.at[1])
    gw_in = pltpu.make_async_copy(gw_hbm, gw_v, local_sem.at[2])
    weights_in = [
        pltpu.make_async_copy(src.at[0], dst, local_sem.at[3 + k])
        for k, (src, dst) in enumerate(((wg_hbm, wg), (wu_hbm, wu), (wd_hbm, wd)))
    ]
    tok_in.start()
    ids_in.start()
    gw_in.start()
    barrier = pltpu.get_barrier_semaphore()
    targets = [{"ep": p} for p in z_peers] + [{"tp": p} for p in x_peers]
    targets += [{"dp": p} for p in c_peers]
    for target in targets:
        pl.semaphore_signal(barrier, inc=1, device_id=target, device_id_type=MESH)
    for copy in weights_in:
        copy.start()

    ids_in.wait()
    gw_in.wait()
    lane = lax.broadcasted_iota(jnp.int32, (rows, LANES), 1)
    diagonal = lax.broadcasted_iota(jnp.int32, (rows, rows), 0)
    diagonal = diagonal == lax.broadcasted_iota(jnp.int32, (rows, rows), 1)

    def upright(row):
        return jnp.sum(jnp.where(diagonal, row, 0.0), axis=1, keepdims=True)

    meta = jnp.zeros((rows, LANES), jnp.float32)
    for k in range(top):
        gate = upright(gw_v[k : k + 1, :])
        high = gate.astype(jnp.bfloat16).astype(jnp.float32)
        middle = (gate - high).astype(jnp.bfloat16).astype(jnp.float32)
        low = gate - high - middle
        named = upright(ids_v[k : k + 1, :].astype(jnp.float32))
        for position, part in enumerate((named, high, middle, low)):
            meta = jnp.where(lane == position * top + k, part, meta)
    xall[x, c, z, :, width:] = meta.astype(jnp.bfloat16)
    tok_in.wait()
    pl.semaphore_wait(barrier, len(targets))

    def remote(src, dst, send, recv, target):
        return pltpu.make_async_remote_copy(
            src_ref=src, dst_ref=dst, send_sem=send, recv_sem=recv,
            device_id=target, device_id_type=MESH,
        )

    def along_z(owner, target):
        block = xall.at[x, c, owner]
        return remote(block, block, az_s.at[target], az_r.at[owner], {"ep": target})

    def along_x(column, owner, target):
        block = xall.at[column, c, owner]
        return remote(
            block, block, ax_s.at[target, owner], ax_r.at[column, owner], {"tp": target}
        )

    def along_c(column, core, owner, target):
        block = xall.at[column, core, owner]
        return remote(
            block, block, ad_s.at[target, column, owner], ad_r.at[core, column, owner],
            {"dp": target},
        )

    sent = []

    def go(copy):
        copy.start()
        sent.append(copy)

    for p in z_peers:
        go(along_z(z, p))
    for p in x_peers:
        go(along_x(x, z, p))
    for p in c_peers:
        go(along_c(x, c, z, p))
    for p in z_peers:
        along_z(p, p).wait_recv()
        for q in x_peers:
            go(along_x(x, p, q))
        for q in c_peers:
            go(along_c(x, c, p, q))

    gathered = ep * dp * rows
    mine = z * dp + c
    loads = jnp.zeros((1, LANES), jnp.float32)
    lanes_all = lax.broadcasted_iota(jnp.int32, (gathered, LANES), 1)

    def apply(column, loads):
        for q in c_peers:
            for owner in [z] + z_peers:
                along_c(column, q, owner, q).wait_recv()
        flat = xall[column].reshape(gathered, width + LANES)
        token_rows = flat[:, :width]
        info = flat[:, width:].astype(jnp.float32)
        scale = jnp.zeros((gathered, 1), jnp.float32)
        for k in range(top):
            named = info[:, k : k + 1].astype(jnp.int32)
            loads = loads + jnp.sum(
                (named == lanes_all).astype(jnp.float32), axis=0, keepdims=True
            )
            gate = info[:, top + k : top + k + 1] + info[:, 2 * top + k : 2 * top + k + 1]
            gate = gate + info[:, 3 * top + k : 3 * top + k + 1]
            scale = scale + jnp.where(named == mine, gate, 0.0)
        gate_value = jnp.dot(token_rows, wg[...], preferred_element_type=jnp.float32)
        up_value = jnp.dot(token_rows, wu[...], preferred_element_type=jnp.float32)
        hidden = gate_value / (1.0 + jnp.exp(-gate_value)) * up_value
        hidden = hidden.astype(jnp.bfloat16)
        for first in range(0, width, STRIP):
            cols = slice(first, first + STRIP)
            value = lax.dot_general(
                hidden, wd[cols, :], (((1,), (1,)), ((), ())),
                preferred_element_type=jnp.float32,
            )
            value = (value * scale).reshape(dp, ep, rows, STRIP)
            resf[column, :, :, :, cols] = value
            resb[column, :, :, :, cols] = value.astype(jnp.bfloat16)
        for q in c_peers:
            go(over_c(column, c, q))
        return loads

    def over_c(column, core, target):
        return remote(
            resb.at[column, target], drecv.at[core, column],
            rd_s.at[target, column], rd_r.at[core, column], {"dp": target},
        )

    def chip_sum(column, owner):
        total = resf[column, c, owner]
        for q in c_peers:
            total = total + drecv[q, column, owner].astype(jnp.float32)
        return total

    def over_x(column, owner, target):
        return remote(
            xsend.at[target, owner], xrecv.at[column, owner],
            rx_s.at[target, owner], rx_r.at[column, owner], {"tp": target},
        )

    def over_z(owner, target):
        return remote(
            zsend.at[target], zrecv.at[owner], rz_s.at[target], rz_r.at[owner],
            {"ep": target},
        )

    for copy in weights_in:
        copy.wait()
    loads = apply(x, loads)
    for p in x_peers:
        for owner in [z] + z_peers:
            along_x(p, owner, p).wait_recv()
            for q in c_peers:
                go(along_c(p, c, owner, q))
    for p in x_peers:
        loads = apply(p, loads)
    loads_ref[...] = jnp.broadcast_to(loads, loads_ref.shape).astype(jnp.int32)

    outward = z_peers[::-1] + [z]
    for p in x_peers:
        for q in c_peers:
            over_c(p, q, q).wait_recv()
        for owner in outward:
            xsend[p, owner] = chip_sum(p, owner).astype(jnp.bfloat16)
            go(over_x(x, owner, p))
    for q in c_peers:
        over_c(x, q, q).wait_recv()
    total = None
    for owner in outward:
        total = chip_sum(x, owner)
        for p in x_peers:
            over_x(p, owner, p).wait_recv()
            total = total + xrecv[p, owner].astype(jnp.float32)
        if owner is not z:
            zsend[owner] = total.astype(jnp.bfloat16)
            go(over_z(z, owner))
    for p in z_peers:
        over_z(p, p).wait_recv()
        total = total + zrecv[p].astype(jnp.float32)
    out_ref[...] = total.astype(out_ref.dtype)
    for copy in sent:
        copy.wait_send()


def fused_layer(tokens, expert_ids, gate_weights, w_gate, w_up, w_down):
    rows, width = tokens.shape
    top = expert_ids.shape[1]
    ep, tp, dp = lax.axis_size("ep"), lax.axis_size("tp"), lax.axis_size("dp")
    experts, hidden_part = ep * dp, w_gate.shape[2]
    sizes = (ep, tp, dp, rows, width, top, experts)
    bf16, f32, dma = jnp.bfloat16, jnp.float32, pltpu.SemaphoreType.DMA
    mixed, loads = pl.pallas_call(
        functools.partial(layer_kernel, sizes),
        out_shape=(
            jax.ShapeDtypeStruct((rows, width), bf16),
            jax.ShapeDtypeStruct((8, LANES), jnp.int32),
        ),
        in_specs=[pl.BlockSpec(memory_space=pl.ANY)] * 6,
        out_specs=[pl.BlockSpec(memory_space=pltpu.VMEM)] * 2,
        scratch_shapes=[
            pltpu.VMEM((tp, dp, ep, rows, width + LANES), bf16),
            pltpu.VMEM((top, rows), jnp.int32),
            pltpu.VMEM((top, rows), f32),
            pltpu.VMEM((width, hidden_part), bf16),
            pltpu.VMEM((width, hidden_part), bf16),
            pltpu.VMEM((width, hidden_part), bf16),
            pltpu.VMEM((tp, dp, ep, rows, width), f32),
            pltpu.VMEM((tp, dp, ep, rows, width), bf16),
            pltpu.VMEM((dp, tp, ep, rows, width), bf16),
            pltpu.VMEM((tp, ep, rows, width), bf16),
            pltpu.VMEM((tp, ep, rows, width), bf16),
            pltpu.VMEM((ep, rows, width), bf16),
            pltpu.VMEM((ep, rows, width), bf16),
            dma((6,)),
            dma((ep,)), dma((ep,)),
            dma((tp, ep)), dma((tp, ep)),
            dma((dp, tp, ep)), dma((dp, tp, ep)),
            dma((dp, tp)), dma((dp, tp)),
            dma((tp, ep)), dma((tp, ep)),
            dma((ep,)), dma((ep,)),
        ],
        compiler_params=pltpu.CompilerParams(
            collective_id=0, has_side_effects=True
        ),
    )(tokens, expert_ids.T, gate_weights.T, w_gate, w_up, w_down)
    return mixed, loads[0, :experts]


def expert_apply(token_rows, gate_part, up_part, down_part):
    gate_value = jnp.dot(token_rows, gate_part, preferred_element_type=jnp.float32)
    up_value = jnp.dot(token_rows, up_part, preferred_element_type=jnp.float32)
    hidden = (jax.nn.silu(gate_value) * up_value).astype(jnp.bfloat16)
    return lax.dot_general(
        hidden, down_part, (((1,), (1,)), ((), ())), preferred_element_type=jnp.float32
    )


def per_device(tokens, expert_ids, gate_weights, w_gate, w_up, w_down):
    tok_rows = tokens.shape[0]
    model_width = tokens.shape[1]
    top_count = expert_ids.shape[1]
    ep_count = lax.axis_size("ep")
    dp_count = lax.axis_size("dp")
    experts = ep_count * dp_count
    capacity = max(2, 2 * tok_rows * top_count // experts)
    if capacity >= tok_rows and experts <= LANES and 4 * top_count <= LANES:
        return fused_layer(tokens, expert_ids, gate_weights, w_gate, w_up, w_down)
    pair_ids = expert_ids.reshape(-1)
    expert_range = jnp.arange(experts, dtype=jnp.int32)
    onehot = (pair_ids[:, None] == expert_range[None, :]).astype(jnp.int32)
    local_counts = jnp.sum(onehot, axis=0).astype(jnp.float32)
    expert_loads = lax.psum(local_counts, ("ep", "tp", "dp")).astype(jnp.int32)
    earlier = (jnp.cumsum(onehot, axis=0) - onehot) * onehot
    slot_ranks = jnp.sum(earlier, axis=1)
    targets = pair_ids * capacity + slot_ranks
    slot_range = jnp.arange(experts * capacity, dtype=jnp.int32)
    selector = jnp.any(
        targets.reshape(tok_rows, top_count)[None, :, :] == slot_range[:, None, None], axis=2
    )
    outgoing = jnp.dot(selector.astype(jnp.bfloat16), tokens, preferred_element_type=jnp.float32)
    outgoing = outgoing.astype(jnp.bfloat16).reshape(experts, capacity, model_width)
    arrived = lax.all_to_all(outgoing, ("ep", "dp"), split_axis=0, concat_axis=0, tiled=True)
    gate_local = w_gate[0]
    up_local = w_up[0]
    down_local = w_down[0]
    fragment = lax.all_gather(arrived, "tp", axis=0, tiled=True)
    flat_rows = fragment.reshape(-1, model_width)
    partial_value = expert_apply(flat_rows, gate_local, up_local, down_local)
    partial_terms = partial_value.reshape(fragment.shape[0], capacity, model_width)
    finished = lax.psum_scatter(partial_terms, "tp", scatter_dimension=0, tiled=True).astype(
        jnp.bfloat16
    )
    returned = lax.all_to_all(finished, ("ep", "dp"), split_axis=0, concat_axis=0, tiled=True)
    returned = returned.reshape(experts * capacity, model_width)
    picked = jnp.take(returned, targets, axis=0).reshape(tok_rows, top_count, model_width)
    mixed = jnp.sum(gate_weights[:, :, None] * picked.astype(jnp.float32), axis=1)
    return (mixed.astype(jnp.bfloat16), expert_loads)


def solution(mesh):
    return jax.shard_map(
        per_device,
        mesh=mesh,
        in_specs=(
            P(("groups", "ep", "tp", "dp"), None),
            P(("groups", "ep", "tp", "dp"), None),
            P(("groups", "ep", "tp", "dp"), None),
            P(("ep", "dp"), None, "tp"),
            P(("ep", "dp"), None, "tp"),
            P(("ep", "dp"), None, "tp"),
        ),
        out_specs=(P(("groups", "ep", "tp", "dp"), None), P("groups")),
        check_vma=False,
    )
```

```python
import functools

import jax
import jax.numpy as jnp
from jax import lax
from jax.experimental import pallas as pl
from jax.experimental.pallas import tpu as pltpu
from jax.sharding import PartitionSpec as P

MESH = pl.DeviceIdType.MESH
LANES = 128
STRIP = 512


def nearest_order(ep_count):
    rows = []
    for own in range(ep_count):
        others = [z for z in range(ep_count) if z != own]
        rows.append(sorted(others, key=lambda z: (abs(z - own), z)))
    return rows


def pick(rows, own, position):
    value = jnp.int32(rows[0][position])
    for index in range(1, len(rows)):
        value = jnp.where(own == index, jnp.int32(rows[index][position]), value)
    return value


def layer_kernel(
    sizes,
    tok_hbm, ids_hbm, gw_hbm, wg_hbm, wu_hbm, wd_hbm,
    out_ref, loads_ref,
    xall, ids_v, gw_v, wg, wu, wd, resf, resb, drecv, xsend, xrecv, zsend, zrecv,
    local_sem, az_s, az_r, ax_s, ax_r, ad_s, ad_r, rd_s, rd_r, rx_s, rx_r, rz_s, rz_r, entered,
):
    ep, tp, dp, rows, width, top, experts = sizes
    z, x, c = lax.axis_index("ep"), lax.axis_index("tp"), lax.axis_index("dp")
    order = nearest_order(ep)
    z_peers = [pick(order, z, k) for k in range(ep - 1)]
    x_peers = [lax.rem(x + k, tp) for k in range(1, tp)]
    c_peers = [lax.rem(c + k, dp) for k in range(1, dp)]

    tok_in = pltpu.make_async_copy(
        tok_hbm, xall.at[x, c, z, :, pl.ds(0, width)], local_sem.at[0]
    )
    ids_in = pltpu.make_async_copy(ids_hbm, ids_v, local_sem.at[1])
    gw_in = pltpu.make_async_copy(gw_hbm, gw_v, local_sem.at[2])
    weights_in = [
        pltpu.make_async_copy(src.at[0], dst, local_sem.at[3 + k])
        for k, (src, dst) in enumerate(((wg_hbm, wg), (wu_hbm, wu), (wd_hbm, wd)))
    ]
    tok_in.start()
    ids_in.start()
    gw_in.start()
    barrier = pltpu.get_barrier_semaphore()
    others = [{"tp": p} for p in x_peers] + [{"dp": p} for p in c_peers]
    for target in others:
        pl.semaphore_signal(barrier, inc=1, device_id=target, device_id_type=MESH)
    has_low, has_high = z > 0, z < ep - 1

    @pl.when(has_low)
    def _():
        pl.semaphore_signal(barrier, inc=1, device_id={"ep": z - 1}, device_id_type=MESH)

    @pl.when(has_high)
    def _():
        pl.semaphore_signal(barrier, inc=1, device_id={"ep": z + 1}, device_id_type=MESH)

    greeted = len(others) + jnp.where(has_low, 1, 0) + jnp.where(has_high, 1, 0)
    for copy in weights_in:
        copy.start()

    ids_in.wait()
    gw_in.wait()
    lane = lax.broadcasted_iota(jnp.int32, (rows, LANES), 1)
    diagonal = lax.broadcasted_iota(jnp.int32, (rows, rows), 0)
    diagonal = diagonal == lax.broadcasted_iota(jnp.int32, (rows, rows), 1)

    def upright(row):
        return jnp.sum(jnp.where(diagonal, row, 0.0), axis=1, keepdims=True)

    meta = jnp.zeros((rows, LANES), jnp.float32)
    for k in range(top):
        gate = upright(gw_v[k : k + 1, :])
        high = gate.astype(jnp.bfloat16).astype(jnp.float32)
        middle = (gate - high).astype(jnp.bfloat16).astype(jnp.float32)
        low = gate - high - middle
        named = upright(ids_v[k : k + 1, :].astype(jnp.float32))
        for position, part in enumerate((named, high, middle, low)):
            meta = jnp.where(lane == position * top + k, part, meta)
    xall[x, c, z, :, width:] = meta.astype(jnp.bfloat16)
    tok_in.wait()
    pl.semaphore_wait(barrier, greeted)

    def remote(src, dst, send, recv, target):
        return pltpu.make_async_remote_copy(
            src_ref=src, dst_ref=dst, send_sem=send, recv_sem=recv,
            device_id=target, device_id_type=MESH,
        )

    def along_z(owner, target):
        block = xall.at[x, c, owner]
        return remote(block, block, az_s.at[target], az_r.at[owner], {"ep": target})

    def along_x(column, owner, target):
        block = xall.at[column, c, owner]
        return remote(
            block, block, ax_s.at[target, owner], ax_r.at[column, owner], {"tp": target}
        )

    def along_c(column, core, owner, target):
        block = xall.at[column, core, owner]
        return remote(
            block, block, ad_s.at[target, column, owner], ad_r.at[core, column, owner],
            {"dp": target},
        )

    sent = []

    def go(copy):
        copy.start()
        sent.append(copy)

    def pass_on(p):
        @pl.when((p - z) * (p - z) > 1)
        def _():
            pl.semaphore_wait(entered.at[p], 1)

        @pl.when((p < z) & has_high)
        def _():
            pl.semaphore_signal(
                entered.at[p], inc=1, device_id={"ep": z + 1}, device_id_type=MESH
            )

        @pl.when((p > z) & has_low)
        def _():
            pl.semaphore_signal(
                entered.at[p], inc=1, device_id={"ep": z - 1}, device_id_type=MESH
            )

    for p in x_peers:
        go(along_x(x, z, p))
    for p in c_peers:
        go(along_c(x, c, z, p))
    for p in z_peers:
        pass_on(p)
        go(along_z(z, p))
    for p in z_peers:
        along_z(p, p).wait_recv()
        for q in x_peers:
            go(along_x(x, p, q))
        for q in c_peers:
            go(along_c(x, c, p, q))

    gathered = ep * dp * rows
    mine = z * dp + c
    loads = jnp.zeros((1, LANES), jnp.float32)
    lanes_all = lax.broadcasted_iota(jnp.int32, (gathered, LANES), 1)

    def apply(column, loads):
        for q in c_peers:
            for owner in [z] + z_peers:
                along_c(column, q, owner, q).wait_recv()
        flat = xall[column].reshape(gathered, width + LANES)
        token_rows = flat[:, :width]
        info = flat[:, width:].astype(jnp.float32)
        scale = jnp.zeros((gathered, 1), jnp.float32)
        for k in range(top):
            named = info[:, k : k + 1].astype(jnp.int32)
            loads = loads + jnp.sum(
                (named == lanes_all).astype(jnp.float32), axis=0, keepdims=True
            )
            gate = info[:, top + k : top + k + 1] + info[:, 2 * top + k : 2 * top + k + 1]
            gate = gate + info[:, 3 * top + k : 3 * top + k + 1]
            scale = scale + jnp.where(named == mine, gate, 0.0)
        gate_value = jnp.dot(token_rows, wg[...], preferred_element_type=jnp.float32)
        up_value = jnp.dot(token_rows, wu[...], preferred_element_type=jnp.float32)
        hidden = gate_value / (1.0 + jnp.exp(-gate_value)) * up_value
        hidden = hidden.astype(jnp.bfloat16)
        for first in range(0, width, STRIP):
            cols = slice(first, first + STRIP)
            value = lax.dot_general(
                hidden, wd[cols, :], (((1,), (1,)), ((), ())),
                preferred_element_type=jnp.float32,
            )
            value = (value * scale).reshape(dp, ep, rows, STRIP)
            resf[column, :, :, :, cols] = value
            resb[column, :, :, :, cols] = value.astype(jnp.bfloat16)
        for q in c_peers:
            go(over_c(column, c, q))
        return loads

    def over_c(column, core, target):
        return remote(
            resb.at[column, target], drecv.at[core, column],
            rd_s.at[target, column], rd_r.at[core, column], {"dp": target},
        )

    def chip_sum(column, owner):
        total = resf[column, c, owner]
        for q in c_peers:
            total = total + drecv[q, column, owner].astype(jnp.float32)
        return total

    def over_x(column, owner, target):
        return remote(
            xsend.at[target, owner], xrecv.at[column, owner],
            rx_s.at[target, owner], rx_r.at[column, owner], {"tp": target},
        )

    def over_z(owner, target):
        return remote(
            zsend.at[target], zrecv.at[owner], rz_s.at[target], rz_r.at[owner],
            {"ep": target},
        )

    for copy in weights_in:
        copy.wait()
    loads = apply(x, loads)
    for p in x_peers:
        for owner in [z] + z_peers:
            along_x(p, owner, p).wait_recv()
            for q in c_peers:
                go(along_c(p, c, owner, q))
    for p in x_peers:
        loads = apply(p, loads)
    loads_ref[...] = jnp.broadcast_to(loads, loads_ref.shape).astype(jnp.int32)

    outward = z_peers[::-1] + [z]
    for p in x_peers:
        for q in c_peers:
            over_c(p, q, q).wait_recv()
        for owner in outward:
            xsend[p, owner] = chip_sum(p, owner).astype(jnp.bfloat16)
            go(over_x(x, owner, p))
    for q in c_peers:
        over_c(x, q, q).wait_recv()
    total = None
    for owner in outward:
        total = chip_sum(x, owner)
        for p in x_peers:
            over_x(p, owner, p).wait_recv()
            total = total + xrecv[p, owner].astype(jnp.float32)
        if owner is not z:
            zsend[owner] = total.astype(jnp.bfloat16)
            go(over_z(z, owner))
    for p in z_peers:
        over_z(p, p).wait_recv()
        total = total + zrecv[p].astype(jnp.float32)
    out_ref[...] = total.astype(out_ref.dtype)
    for copy in sent:
        copy.wait_send()


def finish_kernel(mixed_ref, loads_ref, out_ref, counts_ref):
    out_ref[...] = mixed_ref[...]
    counts_ref[...] = loads_ref[0, : counts_ref.shape[0]]


def fused_layer(tokens, expert_ids, gate_weights, w_gate, w_up, w_down):
    rows, width = tokens.shape
    top = expert_ids.shape[1]
    ep, tp, dp = lax.axis_size("ep"), lax.axis_size("tp"), lax.axis_size("dp")
    experts, hidden_part = ep * dp, w_gate.shape[2]
    sizes = (ep, tp, dp, rows, width, top, experts)
    bf16, f32, dma = jnp.bfloat16, jnp.float32, pltpu.SemaphoreType.DMA
    mixed, loads = pl.pallas_call(
        functools.partial(layer_kernel, sizes),
        out_shape=(
            jax.ShapeDtypeStruct((rows, width), bf16),
            jax.ShapeDtypeStruct((8, LANES), jnp.int32),
        ),
        in_specs=[pl.BlockSpec(memory_space=pl.ANY)] * 6,
        out_specs=[pl.BlockSpec(memory_space=pltpu.VMEM)] * 2,
        scratch_shapes=[
            pltpu.VMEM((tp, dp, ep, rows, width + LANES), bf16),
            pltpu.VMEM((top, rows), jnp.int32),
            pltpu.VMEM((top, rows), f32),
            pltpu.VMEM((width, hidden_part), bf16),
            pltpu.VMEM((width, hidden_part), bf16),
            pltpu.VMEM((width, hidden_part), bf16),
            pltpu.VMEM((tp, dp, ep, rows, width), f32),
            pltpu.VMEM((tp, dp, ep, rows, width), bf16),
            pltpu.VMEM((dp, tp, ep, rows, width), bf16),
            pltpu.VMEM((tp, ep, rows, width), bf16),
            pltpu.VMEM((tp, ep, rows, width), bf16),
            pltpu.VMEM((ep, rows, width), bf16),
            pltpu.VMEM((ep, rows, width), bf16),
            dma((6,)),
            dma((ep,)), dma((ep,)),
            dma((tp, ep)), dma((tp, ep)),
            dma((dp, tp, ep)), dma((dp, tp, ep)),
            dma((dp, tp)), dma((dp, tp)),
            dma((tp, ep)), dma((tp, ep)),
            dma((ep,)), dma((ep,)),
            pltpu.SemaphoreType.REGULAR((ep,)),
        ],
        compiler_params=pltpu.CompilerParams(
            collective_id=0, has_side_effects=True
        ),
    )(tokens, expert_ids.T, gate_weights.T, w_gate, w_up, w_down)
    return pl.pallas_call(
        finish_kernel,
        out_shape=(
            jax.ShapeDtypeStruct((rows, width), bf16),
            jax.ShapeDtypeStruct((experts,), jnp.int32),
        ),
        in_specs=[pl.BlockSpec(memory_space=pltpu.VMEM)] * 2,
        out_specs=[pl.BlockSpec(memory_space=pltpu.VMEM)] * 2,
        compiler_params=pltpu.CompilerParams(vmem_limit_bytes=4 * 1024 * 1024),
    )(mixed, loads)


def expert_apply(token_rows, gate_part, up_part, down_part):
    gate_value = jnp.dot(token_rows, gate_part, preferred_element_type=jnp.float32)
    up_value = jnp.dot(token_rows, up_part, preferred_element_type=jnp.float32)
    hidden = (jax.nn.silu(gate_value) * up_value).astype(jnp.bfloat16)
    return lax.dot_general(
        hidden, down_part, (((1,), (1,)), ((), ())), preferred_element_type=jnp.float32
    )


def per_device(tokens, expert_ids, gate_weights, w_gate, w_up, w_down):
    tok_rows = tokens.shape[0]
    model_width = tokens.shape[1]
    top_count = expert_ids.shape[1]
    ep_count = lax.axis_size("ep")
    dp_count = lax.axis_size("dp")
    experts = ep_count * dp_count
    capacity = max(2, 2 * tok_rows * top_count // experts)
    if capacity >= tok_rows and experts <= LANES and 4 * top_count <= LANES:
        return fused_layer(tokens, expert_ids, gate_weights, w_gate, w_up, w_down)
    pair_ids = expert_ids.reshape(-1)
    expert_range = jnp.arange(experts, dtype=jnp.int32)
    onehot = (pair_ids[:, None] == expert_range[None, :]).astype(jnp.int32)
    local_counts = jnp.sum(onehot, axis=0).astype(jnp.float32)
    expert_loads = lax.psum(local_counts, ("ep", "tp", "dp")).astype(jnp.int32)
    earlier = (jnp.cumsum(onehot, axis=0) - onehot) * onehot
    slot_ranks = jnp.sum(earlier, axis=1)
    targets = pair_ids * capacity + slot_ranks
    slot_range = jnp.arange(experts * capacity, dtype=jnp.int32)
    selector = jnp.any(
        targets.reshape(tok_rows, top_count)[None, :, :] == slot_range[:, None, None], axis=2
    )
    outgoing = jnp.dot(selector.astype(jnp.bfloat16), tokens, preferred_element_type=jnp.float32)
    outgoing = outgoing.astype(jnp.bfloat16).reshape(experts, capacity, model_width)
    arrived = lax.all_to_all(outgoing, ("ep", "dp"), split_axis=0, concat_axis=0, tiled=True)
    gate_local = w_gate[0]
    up_local = w_up[0]
    down_local = w_down[0]
    fragment = lax.all_gather(arrived, "tp", axis=0, tiled=True)
    flat_rows = fragment.reshape(-1, model_width)
    partial_value = expert_apply(flat_rows, gate_local, up_local, down_local)
    partial_terms = partial_value.reshape(fragment.shape[0], capacity, model_width)
    finished = lax.psum_scatter(partial_terms, "tp", scatter_dimension=0, tiled=True).astype(
        jnp.bfloat16
    )
    returned = lax.all_to_all(finished, ("ep", "dp"), split_axis=0, concat_axis=0, tiled=True)
    returned = returned.reshape(experts * capacity, model_width)
    picked = jnp.take(returned, targets, axis=0).reshape(tok_rows, top_count, model_width)
    mixed = jnp.sum(gate_weights[:, :, None] * picked.astype(jnp.float32), axis=1)
    return (mixed.astype(jnp.bfloat16), expert_loads)


def solution(mesh):
    return jax.shard_map(
        per_device,
        mesh=mesh,
        in_specs=(
            P(("groups", "ep", "tp", "dp"), None),
            P(("groups", "ep", "tp", "dp"), None),
            P(("groups", "ep", "tp", "dp"), None),
            P(("ep", "dp"), None, "tp"),
            P(("ep", "dp"), None, "tp"),
            P(("ep", "dp"), None, "tp"),
        ),
        out_specs=(P(("groups", "ep", "tp", "dp"), None), P("groups")),
        check_vma=False,
    )
```
